32 devices in a mesh: row: 4 (over z), col: 8 (over y, x, core).
Axes of the slice: x: 2, y: 2, z: 4, core: 2. Of those that a mesh axis runs over, the one named last changes fastest.
Arguments:
- ainv_anc: bfloat16 [12288, 12288], P('row', 'col'), may hold values from -6 to 6
- l_panel: bfloat16 [1536, 12288], P('col', 'row'), may hold values from -0.109375 to 0.109375
- diag_inv: float32 [1536, 768], P('col', 'row'), may hold values from -6 to 6
- struct_mask: int32 [2, 96], replicated, may hold values 0 or 1
- pieces: float32 [1536, 32, 128], P(('row', 'col')), may hold values from -6 to 6
- tile_owner: int32 [1536, 1], P(('row', 'col')), may hold values from 0 to 31; in each aligned block of 48 rows (0 to 47, 48 to 95, ...) at most 3 rows name the same one
Outputs:
- ainv_upper: bfloat16 [1536, 12288], P('col', 'row')
- ainv_diag: float32 [1536, 768], P('col', 'row')
- moved: float32 [3072, 32, 128], P(('row', 'col'))
The draws below stay inside these ranges and needn't reach their ends.
Inputs may be any that keep to these rules, and one draw needn't show every extreme that they name: `tile_owner`: among the 48 pieces of one device no owner is named more than 3 times, a bound that some block reaches.
All inputs are finite; a program needn't handle non-finite values.
Results may differ from the reference program's by a relative error of at most 0.015.
Values may be sent and summed in bfloat16 or wider, within the bound.
A program may use at most 128 MiB of HBM per device.

```python
import math
import jax
import jax.numpy as jnp
import numpy as np
from jax import lax

W = 768
NS = 2
AB = 128
SLOT = 3
TR = 32
TC = 128
ORDER = 12288
PANEL = 1536
NBLK = 96
TPD = 48
PIECES = 1536
N_ROW = 4
N_COL = 8
DEVICES = 32


def touch_ends(values, key, least, top_value):
    dims = values.shape
    index_at = [jax.random.randint(jax.random.fold_in(key, axis), (), 0, dims[axis]) for axis in range(len(dims))]
    values = values.at[tuple(index_at)].set(least)
    longest = dims.index(max(dims))
    index_at[longest] = (index_at[longest] + 1) % dims[longest]
    return values.at[tuple(index_at)].set(top_value)


def raised(values, own_key, source, target, parts, factor):
    def block_of(position):
        return (jnp.arange(values.shape[position]) // (values.shape[position] // parts)).reshape((-1,) + (1,) * (values.ndim - 1 - position))

    one_side = jax.random.permutation(own_key, parts)[block_of(target)]
    second = (block_of(target) + parts // 2) % parts
    return jnp.where((block_of(source) == one_side) | (block_of(source) == second), factor * values, values)


def shard_levels(key, extent, cuts, smallest, top_value):
    def one(position, parts):
        heights = jax.random.uniform(jax.random.fold_in(jax.random.fold_in(key, 6), position), (parts,), jnp.float32, smallest / len(cuts), top_value / len(cuts))
        return jnp.repeat(jnp.exp(heights), extent[position] // parts).reshape((-1,) + (1,) * (len(extent) - position - 1))

    loudness = one(*cuts[0])
    for cut in cuts[1:]:
        loudness = loudness * one(*cut)
    return loudness


def shared_out(key, own, number, rows, count, top, bound, skew):
    sequence = jax.random.permutation(key, count)
    crowded, common = load_shares(count, rows * top, bound, skew, True), load_shares(count, rows * top, bound, skew, False)
    places = jnp.arange(count)

    def named(tallies, offset_by):
        used = int((tallies > 0).sum())
        fixed = max(1, used // 4)
        passed = fixed + (places - fixed + offset_by * (used - fixed)) % max(1, count - fixed)
        return jnp.zeros((count,), jnp.int32).at[sequence[jnp.where(places < fixed, places, passed)]].set(jnp.asarray(tallies, jnp.int32))

    tallies = jnp.where(number % 4 == 0, named(crowded, number // 4), named(common, number - number // 4 - 1))
    mixed = jax.random.permutation(jax.random.fold_in(own, 3), count)
    donor, receiver = mixed[0:count // 2 * 2:2], mixed[1:count // 2 * 2:2]
    slack = jnp.minimum(tallies[donor] - 1, bound - tallies[receiver]) // 2
    slack = jnp.where((donor == sequence[0]) | (receiver == sequence[0]) | (tallies[receiver] == 0), 0, jnp.maximum(slack, 0))
    passed = jax.random.randint(jax.random.fold_in(own, 4), (count // 2,), 0, 1 << 20) % (slack + 1)
    tallies = tallies.at[donor].add(-passed).at[receiver].add(passed)
    members = jnp.searchsorted(jnp.cumsum(tallies), jnp.arange(rows * top), side="right").astype(jnp.int32)
    listing = members.reshape(top, rows).T
    listing = listing[jax.random.permutation(jax.random.fold_in(own, 1), rows)]
    offset_by = jax.random.randint(jax.random.fold_in(own, 2), (rows, 1), 0, top)
    return jnp.take_along_axis(listing, (jnp.arange(top)[None, :] + offset_by) % top, axis=1)


def load_shares(count, total, reach, lean, full):
    loads = [(1 << 20) // math.isqrt(grade ** lean) + 1 for grade in range(1, count + 1)]
    largest = reach if full else min(reach, max(-(-total // count), total * loads[0] // sum(loads)))
    least = 1 if total - largest >= count - 1 else 0
    holding, spare = [largest] + [least] * (count - 1), total - largest - least * (count - 1)
    while spare > 0:
        free = [i for i in range(1, count) if holding[i] < largest] or [i for i in range(1, count) if holding[i] < reach]
        pool, remaining = sum([loads[i] for i in free]), spare
        for i in free:
            more = min(reach - holding[i], max(1, remaining * loads[i] // pool), spare)
            holding[i] = holding[i] + more
            spare = spare - more
    return np.array(holding)


def noise(key, shape, deviation, most, cuts=(), held_as=jnp.bfloat16):
    result = jax.random.normal(key, shape, jnp.float32) * deviation
    if len(cuts) > 0:
        result = shard_levels(key, shape, cuts, -0.22, 0.18) * result
    return jnp.clip(result, min=-most, max=most).astype(held_as)


def noise_with(rng, extent, width, bound, cuts, heavy, held_as=jnp.bfloat16):
    values = width * jax.random.normal(rng, extent, jnp.float32)
    if cuts:
        values = values * shard_levels(rng, extent, cuts, -0.22, 0.18)
    return jnp.clip(raised(values, jax.random.fold_in(rng, 3), *heavy), -bound, bound).astype(held_as)


def setup_inputs(seed: int = 0) -> dict:
    seeds = jax.random.split(jax.random.key(seed), 7)
    ainv_anc = noise(seeds[0], (ORDER, ORDER), 1.0, 6.0, ((0, 4), (1, 8)))
    l_panel = noise_with(seeds[1], (PANEL, ORDER), (ORDER // 2) ** -0.5, 0.109375, ((0, 8), (1, 4)), (1, 0, 8, 2.0))
    diag_inv = noise(seeds[2], (PANEL, W), 1.0, 6.0, ((0, 8), (1, 4)), jnp.float32)
    struct_mask = touch_ends((jax.random.randint(seeds[3], (NS, NBLK), 0, 2) < 1).astype(jnp.int32), jax.random.fold_in(seeds[3], 1), 0, 1)
    pieces = noise(seeds[4], (PIECES, TR, TC), 1.0, 6.0, ((0, 32),), jnp.float32)
    tile_owner_keys = jax.random.split(jax.random.fold_in(seeds[5], 1), PIECES // TPD)
    tile_owner_turns = jax.random.permutation(jax.random.fold_in(seeds[5], 3), PIECES // TPD)
    tile_owner = jax.vmap(lambda own, number: shared_out(jax.random.fold_in(seeds[5], 2), own, number, TPD, DEVICES, 1, SLOT, 2))(tile_owner_keys, tile_owner_turns).reshape((PIECES, 1))
    return dict(ainv_anc=ainv_anc, l_panel=l_panel, diag_inv=diag_inv, struct_mask=struct_mask, pieces=pieces, tile_owner=tile_owner)


def mask_panel(l_panel, struct_mask):
    blocks = jnp.repeat(struct_mask, AB, axis=1)
    keep = blocks[:, None, :] > 0
    shaped = l_panel.reshape(NS, W, ORDER)
    masked = jnp.where(keep, shaped, jnp.zeros_like(shaped))
    return masked.reshape(NS * W, ORDER), keep


def reference(ainv_anc, l_panel, diag_inv, struct_mask, pieces, tile_owner):
    masked_panel, keep = mask_panel(l_panel, struct_mask)
    group_width = ORDER // N_COL

    def add_group(index, total):
        begin = (index * group_width).astype(jnp.int32)
        panel_cols = lax.dynamic_slice_in_dim(masked_panel, begin, group_width, 1)
        inverse_cols = lax.dynamic_slice_in_dim(ainv_anc, begin, group_width, 1)
        term = lax.dot_general(panel_cols, inverse_cols, (((1,), (1,)), ((), ())), preferred_element_type=jnp.float32)
        rounded = lax.optimization_barrier(term.astype(jnp.bfloat16))
        return total + rounded.astype(jnp.float32)

    product = lax.fori_loop(0, N_COL, add_group, jnp.zeros((NS * W, ORDER), jnp.float32))
    shaped = product.reshape(NS, W, ORDER)
    upper_rows = jnp.where(keep, -shaped, jnp.zeros_like(shaped)).reshape(NS * W, ORDER).astype(jnp.bfloat16)
    diag_blocks = []
    for supernode in range(NS):
        upper_part = upper_rows[supernode * W:(supernode + 1) * W]
        panel_part = masked_panel[supernode * W:(supernode + 1) * W]
        diag_blocks.append(lax.dot_general(upper_part, panel_part, (((1,), (1,)), ((), ())), preferred_element_type=jnp.float32))
    ainv_diag = diag_inv - jnp.concatenate(diag_blocks, axis=0)
    devices_all = N_ROW * N_COL
    owners = tile_owner[:, 0].reshape(devices_all, TPD)
    onehot = (owners[:, :, None] == jnp.arange(devices_all, dtype=jnp.int32)[None, None, :]).astype(jnp.int32)
    earlier = jnp.cumsum(onehot, axis=1) - onehot
    rank_in_dest = jnp.sum(earlier * onehot, axis=2)
    source = jnp.arange(devices_all, dtype=jnp.int32)[:, None]
    slot_index = ((owners * devices_all + source) * SLOT + rank_in_dest).reshape(-1).astype(jnp.int32)
    moved = jnp.zeros((devices_all * devices_all * SLOT, TR, TC), jnp.float32).at[slot_index].set(pieces)
    return upper_rows, ainv_diag, moved
```

```python
import functools

import jax
import jax.numpy as jnp
from jax import lax
from jax.experimental import pallas as pl
from jax.experimental.pallas import tpu as pltpu
from jax.sharding import PartitionSpec as P

W = 768
AB = 128
SLOT = 3
TILES = 3
MESH = pl.DeviceIdType.MESH


def flip(index, mask):
    out = index
    bit = 1
    while bit <= mask:
        if mask & bit:
            out = out + bit - 2 * bit * ((index // bit) % 2)
        bit *= 2
    return out


def differ(a, b, size):
    out = 0
    bit = 1
    while bit < size:
        out = out + ((a // bit + b // bit) % 2) * bit
        bit *= 2
    return out


def bit_order(size):
    bits = [1 << i for i in range(size.bit_length() - 1)]
    return bits[1:][::-1] + bits[:1]


def kernel(
    R, C, x_ref, ainv_hbm, keep_ref, diag_ref, upper_ref, out_diag_ref,
    ainv_ref, zbuf, gbuf, pbuf, rbuf, dbuf, dsend, drecv,
    asem, zr, zsu, zsd, ps, pr, rs, rr, gs, gr, es, er,
):
    T, ratio, nt, cw = x_ref.shape
    n = T * nt
    LR = ratio * cw
    peers = W // n
    r = lax.axis_index("row")
    c = lax.axis_index("col")
    own = c % peers

    load = pltpu.make_async_copy(ainv_hbm, ainv_ref, asem)
    load.start()

    barrier = pltpu.get_barrier_semaphore()
    for d in range(1, R):
        pl.semaphore_signal(barrier, inc=1, device_id=((r + d) % R, c), device_id_type=MESH)
    for j in range(1, C):
        pl.semaphore_signal(barrier, inc=1, device_id=(r, flip(c, j)), device_id_type=MESH)
    pl.semaphore_wait(barrier, R + C - 2)

    def z_copy(t, g, src, step):
        sems = zsu if step > 0 else zsd
        return pltpu.make_async_remote_copy(
            src_ref=src, dst_ref=zbuf.at[t, g], send_sem=sems.at[t, g], recv_sem=zr.at[t, g],
            device_id=(r + step, c), device_id_type=MESH,
        )

    def p_copy(t, g, src):
        j = differ(c, g, C)
        return pltpu.make_async_remote_copy(
            src_ref=src, dst_ref=gbuf.at[t, j], send_sem=ps.at[t, g], recv_sem=pr.at[t, j],
            device_id=(r, g), device_id_type=MESH,
        )

    def spread(t, g, src):
        @pl.when(g == c)
        def _():
            gbuf[t, 0] = src[...]

        @pl.when(g != c)
        def _():
            p_copy(t, g, src).start()

    def z_own(t):
        for h in range(ratio):
            g = r * ratio + h
            src = x_ref.at[t, h]

            @pl.when(r + 1 < R)
            def _():
                z_copy(t, g, src, 1).start()

            @pl.when(r > 0)
            def _():
                z_copy(t, g, src, -1).start()

            spread(t, g, src)

    def z_step(t, d):
        for h in range(ratio):
            below = (r - d) * ratio + h

            @pl.when(r - d >= 0)
            def _():
                src = zbuf.at[t, below]
                z_copy(t, below, src, 1).wait_recv()

                @pl.when(r + 1 < R)
                def _():
                    z_copy(t, below, src, 1).start()

                spread(t, below, src)

            above = (r + d) * ratio + h

            @pl.when(r + d < R)
            def _():
                src = zbuf.at[t, above]
                z_copy(t, above, src, -1).wait_recv()

                @pl.when(r > 0)
                def _():
                    z_copy(t, above, src, -1).start()

                spread(t, above, src)

    def z_phase(t):
        z_own(t)
        for d in range(1, R):
            z_step(t, d)

    def g_copy(rel, bit):
        where = flip(own, rel)
        return pltpu.make_async_remote_copy(
            src_ref=x_ref if rel == 0 else dbuf.at[where], dst_ref=dbuf.at[where],
            send_sem=gs.at[(rel ^ bit)], recv_sem=gr.at[(rel ^ bit)],
            device_id=(r, flip(c, bit)), device_id_type=MESH,
        )

    gather_plan = []
    held = [0]
    for bit in bit_order(peers):
        gather_plan.append((bit, list(held)))
        held = held + [j ^ bit for j in held]

    def g_start(stage):
        bit, have = gather_plan[stage]
        for j in have:
            g_copy(j, bit).start()

    def g_wait(stage):
        bit, have = gather_plan[stage]
        for j in have:
            g_copy(j, bit).wait()

    reduce_plan = []
    live = list(range(C))
    base = 0
    bits = bit_order(C)
    for bit in bits[-1:] + bits[:-1]:
        keep = [j for j in live if not j & bit]
        reduce_plan.append((bit, keep, base))
        base += len(keep)
        live = keep

    def r_copy(t, stage, j):
        bit, keep, start = reduce_plan[stage]
        slot = start + keep.index(j & ~bit)
        return pltpu.make_async_remote_copy(
            src_ref=pbuf.at[t, j | bit], dst_ref=rbuf.at[t, slot],
            send_sem=rs.at[t, slot], recv_sem=rr.at[t, slot],
            device_id=(r, flip(c, bit)), device_id_type=MESH,
        ), slot

    def multiply(t):
        for j in range(1, C):
            pltpu.make_async_remote_copy(
                src_ref=gbuf.at[t, j], dst_ref=gbuf.at[t, j], send_sem=ps.at[t, 0],
                recv_sem=pr.at[t, j], device_id=(r, c), device_id_type=MESH,
            ).wait_recv()
        step = 256

        def body(i, carry):
            cols = pl.ds(pl.multiple_of(i * step, step), step)
            got = lax.dot_general(
                gbuf[t].reshape(C * nt, cw), ainv_ref[cols, :], (((1,), (1,)), ((), ())),
                preferred_element_type=jnp.float32,
            )
            pbuf[t, :, :, cols] = got.astype(jnp.bfloat16).reshape(C, nt, step)
            return carry

        lax.fori_loop(0, LR // step, body, 0)
        for j in reduce_plan[0][1][::-1]:
            r_copy(t, 0, j)[0].start()

    def combine(t, stage):
        bit = reduce_plan[stage + 1][0]
        keep = reduce_plan[stage][1]
        for j in sorted(keep, key=lambda v: (0 if v & bit else 1, -v)):
            copy, slot = r_copy(t, stage, j)
            copy.wait_recv()
            pbuf[t, j] = (
                pbuf[t, j].astype(jnp.float32) + rbuf[t, slot].astype(jnp.float32)
            ).astype(jnp.bfloat16)
            if j & bit:
                r_copy(t, stage + 1, j)[0].start()

    def finish(t):
        copy, slot = r_copy(t, len(reduce_plan) - 1, 0)
        copy.wait_recv()
        total = pbuf[t, 0].astype(jnp.float32) + rbuf[t, slot].astype(jnp.float32)
        upper_ref[t * nt:(t + 1) * nt, :] = jnp.where(
            keep_ref[...] > 0, -total, jnp.zeros_like(total)
        ).astype(jnp.bfloat16)

    stages = len(reduce_plan)
    z_phase(0)
    g_start(0)
    dbuf[own] = x_ref[...]
    load.wait()
    for t in range(T):
        if t + 1 < T:
            z_phase(t + 1)
        multiply(t)
        if t >= 1:
            for s in range(1, stages - 1):
                combine(t - 1, s)
        combine(t, 0)
        if t + 1 < len(gather_plan) + 0 and t < len(gather_plan):
            g_wait(t)
            g_start(t + 1)
    for s in range(1, stages - 1):
        combine(T - 1, s)
    for t in range(T - 1):
        finish(t)
    done = min(T, len(gather_plan) - 1)
    for s in range(done, len(gather_plan)):
        if s > done:
            g_start(s)
        g_wait(s)
    finish(T - 1)

    def e_copy(d):
        return pltpu.make_async_remote_copy(
            src_ref=dsend.at[d - 1], dst_ref=drecv.at[d - 1],
            send_sem=es.at[d - 1], recv_sem=er.at[d - 1],
            device_id=((r + d) % R, c), device_id_type=MESH,
        )

    def part(target):
        got = jnp.zeros((n, n), jnp.float32)
        for h in range(ratio):
            got += lax.dot_general(
                upper_ref[:, h * cw:(h + 1) * cw], dbuf[target, :, h].reshape(n, cw),
                (((1,), (1,)), ((), ())), preferred_element_type=jnp.float32,
            )
        return got

    for d in range(R - 1, 0, -1):
        dsend[d - 1] = part((r + d) % R).astype(jnp.bfloat16)
        e_copy(d).start()
    total = part(r)
    for d in range(1, R):
        e_copy(d).wait_recv()
        total = total + drecv[d - 1].astype(jnp.float32)
    out_diag_ref[...] = diag_ref[...] - total
    for d in range(1, R):
        e_copy(d).wait_send()

    for t in range(T):
        for g in range(C):
            src = zbuf.at[t, g]

            @pl.when(jnp.logical_and(r + 1 < R, r >= g // ratio))
            def _():
                z_copy(t, g, src, 1).wait_send()

            @pl.when(jnp.logical_and(r > 0, r <= g // ratio))
            def _():
                z_copy(t, g, src, -1).wait_send()

            @pl.when(c != g)
            def _():
                p_copy(t, g, src).wait_send()

        for s in range(stages):
            for j in reduce_plan[s][1]:
                r_copy(t, s, j)[0].wait_send()


def local(ainv_anc, l_panel, diag_inv, struct_mask, pieces, tile_owner):
    R = lax.axis_size("row")
    C = lax.axis_size("col")
    row_index = lax.axis_index("row")
    col_index = lax.axis_index("col")
    n, LR = l_panel.shape
    cw = ainv_anc.shape[1]
    ratio = LR // cw
    nt = n // TILES
    peers = W // n
    supernode = col_index * n // W
    block_count = LR // AB
    keep_blocks = lax.dynamic_slice(
        struct_mask, (supernode, row_index * block_count), (1, block_count)
    )
    keep_rows = jnp.broadcast_to(keep_blocks[:, :, None], (1, block_count, AB)).reshape(1, LR)
    masked = jnp.where(keep_rows > 0, l_panel, jnp.zeros_like(l_panel))
    x = masked.reshape(TILES, nt, ratio, cw).transpose(0, 2, 1, 3)

    devices_all = R * C
    owners = tile_owner[:, 0]
    onehot = (owners[:, None] == jnp.arange(devices_all, dtype=jnp.int32)[None, :]).astype(
        jnp.int32
    )
    earlier = jnp.cumsum(onehot, axis=0) - onehot
    rank_in_dest = jnp.sum(earlier * onehot, axis=1)
    slot_index = owners * SLOT + rank_in_dest
    tr, tc = pieces.shape[1:]
    buffer = jnp.zeros((devices_all * SLOT, tr, tc), jnp.float32).at[slot_index].set(pieces)
    arrived = lax.all_to_all(
        buffer.reshape(devices_all, SLOT, tr, tc).astype(jnp.bfloat16),
        ("row", "col"), split_axis=0, concat_axis=0, tiled=True,
    ).astype(jnp.float32)
    moved = arrived.reshape(devices_all * SLOT, tr, tc)

    vm = pl.BlockSpec(memory_space=pltpu.VMEM)
    bf = jnp.bfloat16
    dma = pltpu.SemaphoreType.DMA
    upper, diag = pl.pallas_call(
        functools.partial(kernel, R, C),
        out_shape=(
            jax.ShapeDtypeStruct((n, LR), bf),
            jax.ShapeDtypeStruct(diag_inv.shape, jnp.float32),
        ),
        in_specs=[vm, pl.BlockSpec(memory_space=pl.ANY), vm, vm],
        out_specs=(vm, vm),
        scratch_shapes=[
            pltpu.VMEM(ainv_anc.shape, bf),
            pltpu.VMEM((TILES, C, nt, cw), bf),
            pltpu.VMEM((TILES, C, nt, cw), bf),
            pltpu.VMEM((TILES, C, nt, LR), bf),
            pltpu.VMEM((TILES, C - 1, nt, LR), bf),
            pltpu.VMEM((peers, TILES, ratio, nt, cw), bf),
            pltpu.VMEM((R - 1, n, n), bf),
            pltpu.VMEM((R - 1, n, n), bf),
            dma,
            dma((TILES, C)),
            dma((TILES, C)),
            dma((TILES, C)),
            dma((TILES, C)),
            dma((TILES, C)),
            dma((TILES, C)),
            dma((TILES, C)),
            dma((peers,)),
            dma((peers,)),
            dma((R - 1,)),
            dma((R - 1,)),
        ],
        compiler_params=pltpu.CompilerParams(
            collective_id=0, has_side_effects=True, vmem_limit_bytes=63 * 2**20
        ),
        cost_estimate=pl.CostEstimate(
            flops=2 * C * n * LR * cw, bytes_accessed=400_000_000, transcendentals=0
        ),
        name="invert",
    )(x, ainv_anc, keep_rows, diag_inv)
    return upper, diag, moved


def solution(mesh):
    in_specs = (
        P("row", "col"),
        P("col", "row"),
        P("col", "row"),
        P(),
        P(("row", "col"), None, None),
        P(("row", "col"), None),
    )
    out_specs = (P("col", "row"), P("col", "row"), P(("row", "col"), None, None))
    return jax.shard_map(local, mesh=mesh, in_specs=in_specs, out_specs=out_specs, check_vma=False)
```
